256 devices in a mesh: replica: 8 (over y, x_lo), fsdp: 32 (over z, x_hi, core).
Axes of the slice: x: 4 (x_hi: 2, x_lo: 2; x = x_hi * 2 + x_lo), y: 4, z: 8, core: 2. Of those that a mesh axis runs over, the one named last changes fastest.
Arguments:
- codes: int32 [8, 8192, 4096], P('replica', None, 'fsdp'), may hold values from -127 to 127
- scales: float32 [8, 32, 8192], P('replica', 'fsdp'), may hold values from 0.002 to 0.03
- master: float32 [8192, 4096], P(('replica', 'fsdp')), may hold values from -6 to 6
- momentum: float32 [8192, 4096], P(('replica', 'fsdp')), may hold values from -6 to 6
Outputs:
- new_master: float32 [8192, 4096], P(('replica', 'fsdp'))
- new_momentum: float32 [8192, 4096], P(('replica', 'fsdp'))
- weights: bfloat16 [8192, 4096], P(None, 'fsdp')
The draws below stay inside these ranges and needn't reach their ends.
All inputs are finite; a program needn't handle non-finite values.
Results may differ from the reference program's by a relative error of at most 0.0075.
Values may be sent and summed in bfloat16 or wider, within the bound.
No kernel may reach another device: no remote copies, remote signals or barrier semaphores. Data moves between devices by JAX's collectives and lax.ppermute only.
A program may use at most 64 MiB of HBM per device.

```python
import math
import jax
import jax.numpy as jnp
from jax import lax

D = 4096
FF = 8192
BLOCK = 128
REPLICAS = 8
N_REPLICA = 8


def place_ends(entries, key, least, high):
    shape = entries.shape
    spot = [jax.random.randint(jax.random.fold_in(key, axis), (), 0, shape[axis]) for axis in range(len(shape))]
    entries = entries.at[tuple(spot)].set(least)
    longest = shape.index(max(shape))
    spot[longest] = (spot[longest] + 1) % shape[longest]
    return entries.at[tuple(spot)].set(high)


def block_scale(stream_key, extent, cuts, low, top_value):
    def one(dim, blocks):
        steps = jax.random.uniform(jax.random.fold_in(jax.random.fold_in(stream_key, 6), dim), (blocks,), jnp.float32, low / len(cuts), top_value / len(cuts))
        return jnp.repeat(jnp.exp(steps), extent[dim] // blocks).reshape((-1,) + (1,) * (len(extent) - dim - 1))

    loudness = one(*cuts[0])
    for cut in cuts[1:]:
        loudness = loudness * one(*cut)
    return loudness


def noise(stream_key, extent, width, limit, split=(), held_as=jnp.bfloat16):
    entries = width * jax.random.normal(stream_key, extent, jnp.float32)
    if split:
        entries = entries * block_scale(stream_key, extent, split, -0.22, 0.18)
    return jnp.clip(entries, -limit, limit).astype(held_as)


def setup_inputs(seed: int = 0) -> dict:
    seeds = jax.random.split(jax.random.key(seed), 5)
    codes = place_ends(jax.random.randint(seeds[0], (REPLICAS, FF, D), -127, 128), jax.random.fold_in(seeds[0], 1), -127, 127).astype(jnp.int32)
    scales = jnp.clip(jnp.exp(math.log(0.03) - 2.70805 * jax.random.uniform(seeds[1], (REPLICAS, D // BLOCK, FF), jnp.float32) ** block_scale(seeds[1], (REPLICAS, D // BLOCK, FF), ((0, 8), (1, 32)), -0.2, 0.2)), 0.002, 0.03)
    master = noise(seeds[2], (FF, D), 1.0, 6.0, ((0, 256),), jnp.float32)
    momentum = noise(seeds[3], (FF, D), 0.5, 6.0, ((0, 256),), jnp.float32)
    return {"codes": codes, "scales": scales, "master": master, "momentum": momentum}


outer_rate = 0.7
momentum_factor = 0.9


def reference(codes, scales, master, momentum):
    def add_worker(replica_index, running):
        quantized = lax.dynamic_index_in_dim(codes, replica_index, 0, keepdims=False).astype(jnp.float32)
        scale_rows = lax.dynamic_index_in_dim(scales, replica_index, 0, keepdims=False)
        block_count = scale_rows.shape[0]
        dequantized = quantized.reshape(FF, block_count, BLOCK) * jnp.transpose(scale_rows)[:, :, None]
        return running + dequantized.reshape(FF, D)

    summed = lax.fori_loop(0, N_REPLICA, add_worker, jnp.zeros((FF, D), jnp.float32))
    mean_delta = summed / N_REPLICA
    new_momentum = momentum_factor * momentum + mean_delta
    new_master = master - outer_rate * (mean_delta + momentum_factor * new_momentum)
    weights = new_master.astype(jnp.bfloat16)
    return (new_master, new_momentum, weights)
```

```python
import jax
import jax.numpy as jnp
from jax import lax
from jax.experimental import pallas as pl
from jax.experimental.pallas import tpu as pltpu
from jax.sharding import PartitionSpec as P


outer_rate = 0.7
momentum_factor = 0.9

ORDERS = ((0, 1, 2), (1, 2, 0), (2, 0, 1))
CUTS = (0, 352, 688, 1024)
SIZES = tuple(CUTS[k + 1] - CUTS[k] for k in range(3))
BLOCK = 1024
TILE = 128


def partner(r, direction):
    y, x = r // 2, r % 2
    if direction == 0:
        y = y ^ 1
    elif direction == 1:
        y = 3 - y
    else:
        x = x ^ 1
    return 2 * y + x


def swap(v, direction):
    return lax.ppermute(v, "replica", [(r, partner(r, direction)) for r in range(8)])


def away(steps):
    r = lax.axis_index("replica")
    y, x = lax.div(r, 2), lax.rem(r, 2)
    if steps[0]:
        y = jnp.bitwise_xor(y, 1)
    if steps[1]:
        y = 3 - y
    if steps[2]:
        x = 1 - x
    return 2 * y + x


def steps_of(k, first, j):
    steps = [0, 0, 0]
    for direction, bit in zip(ORDERS[k], (first, j // 2, j % 2)):
        steps[direction] = bit
    return steps


def dequant_kernel(first):
    def kernel(codes, scales, *refs):
        outs, buffers, sems = refs[:3], refs[3:6], refs[6]
        copies = []
        for k in range(3):
            for j in range(4):
                block = away(steps_of(k, first, j))
                start = pl.multiple_of(block * BLOCK + CUTS[k], 16)
                copy = pltpu.make_async_copy(
                    codes.at[pl.ds(start, SIZES[k])], buffers[k].at[j], sems.at[k, j]
                )
                copy.start()
                copies.append((k, j, block, copy))
        for k, j, block, copy in copies:
            copy.wait()
            low = CUTS[k]
            while low < CUTS[k + 1]:
                tile = low // TILE
                high = min((tile + 1) * TILE, CUTS[k + 1])
                row = scales[pl.ds(block * (BLOCK // TILE) + tile, 1), :]
                factor = jnp.transpose(jnp.broadcast_to(row, (TILE, TILE)))
                factor = factor[low - tile * TILE : high - tile * TILE]
                here = pl.ds(low - CUTS[k], high - low)
                values = buffers[k][j, here, :].astype(jnp.float32) * factor
                outs[k][j, here, :] = values.astype(outs[k].dtype)
                low = high

    return kernel


def dequant(codes, scales, first):
    return pl.pallas_call(
        dequant_kernel(first),
        out_shape=[pltpu.VMEM((4, n, 128), jnp.bfloat16) for n in SIZES],
        in_specs=[pl.BlockSpec(memory_space=pl.ANY), pl.BlockSpec(memory_space=pltpu.VMEM)],
        out_specs=[pl.BlockSpec(memory_space=pltpu.VMEM)] * 3,
        scratch_shapes=[pltpu.VMEM((4, n, 128), jnp.int32) for n in SIZES]
        + [pltpu.SemaphoreType.DMA((3, 4))],
        compiler_params=pltpu.CompilerParams(vmem_limit_bytes=8 << 20),
    )(codes, scales)


def place_kernel(first, aliased):
    def kernel(*refs):
        pieces, (out, sems) = refs[aliased : aliased + 3], refs[aliased + 3 :]
        copies = []
        for k in range(3):
            for j in range(4):
                start = pl.multiple_of(away(steps_of(k, first, j)) * BLOCK + CUTS[k], 16)
                copies.append(
                    pltpu.make_async_copy(
                        pieces[k].at[j], out.at[pl.ds(start, SIZES[k])], sems.at[k, j]
                    )
                )
        for copy in copies:
            copy.start()
        for copy in copies:
            copy.wait()

    return kernel


def place(pieces, first, out):
    aliased = 0 if out is None else 1
    return pl.pallas_call(
        place_kernel(first, aliased),
        out_shape=jax.ShapeDtypeStruct((8 * BLOCK, 128), jnp.bfloat16),
        in_specs=[pl.BlockSpec(memory_space=pl.ANY)] * aliased
        + [pl.BlockSpec(memory_space=pltpu.VMEM)] * 3,
        out_specs=pl.BlockSpec(memory_space=pl.ANY),
        scratch_shapes=[pltpu.SemaphoreType.DMA((3, 4))],
        input_output_aliases={0: 0} if aliased else {},
        compiler_params=pltpu.CompilerParams(vmem_limit_bytes=4 << 20),
    )(
        *([] if out is None else [out]),
        *[pltpu.with_memory_space_constraint(v, pltpu.VMEM) for v in pieces],
    )


def step(codes, scales, master, momentum):
    f32, bf16 = jnp.float32, jnp.bfloat16
    codes, scales = codes.reshape(8 * BLOCK, 128), scales.reshape(8 * BLOCK // TILE, TILE)
    sent = dequant(codes, scales, 1)
    got = []
    for k in range(3):
        got.append(swap(sent[k], ORDERS[k][0]))

    master_early, momentum_early = lax.optimization_barrier((master, momentum))
    q = master_early - (outer_rate * momentum_factor * momentum_factor) * momentum_early
    q = q.astype(bf16)
    q_columns = lax.all_to_all(q, "fsdp", split_axis=1, concat_axis=0, tiled=True)

    kept = dequant(codes, scales, 0)
    held = list(kept)
    for s in (1, 2):
        for k in range(3):
            v = held[k].astype(f32) + got[k].astype(f32)
            middle = v.shape[0] // 2
            got[k] = swap(v[middle:].astype(bf16), ORDERS[k][s])
            held[k] = v[:middle]
    total = [held[k][0] + got[k][0].astype(f32) for k in range(3)]

    weights = []
    for k in range(3):
        columns = q_columns[CUTS[k] : CUTS[k + 1]].astype(f32)
        w = columns - (outer_rate * (1 + momentum_factor) / 8) * total[k]
        weights.append(w.astype(bf16)[None])
    for s in (2, 1):
        for k in range(3):
            weights[k] = jnp.concatenate([weights[k], swap(weights[k], ORDERS[k][s])])
    others = []
    for k in range(3):
        others.append(swap(weights[k], ORDERS[k][0]))

    summed = jnp.concatenate(total).astype(bf16)
    summed = lax.all_to_all(summed, "fsdp", split_axis=0, concat_axis=1, tiled=True)
    mean = summed.astype(f32) / 8
    new_momentum = momentum_factor * momentum + mean
    new_master = master - outer_rate * (mean + momentum_factor * new_momentum)

    out = place(weights, 0, None)
    out = place(others, 1, out)
    return (new_master, new_momentum, out)


def solution(mesh):
    return jax.shard_map(
        step,
        mesh=mesh,
        in_specs=(
            P("replica", None, "fsdp"),
            P("replica", "fsdp", None),
            P(("replica", "fsdp"), None),
            P(("replica", "fsdp"), None),
        ),
        out_specs=(P(("replica", "fsdp"), None), P(("replica", "fsdp"), None), P(None, "fsdp")),
        check_vma=False,
    )
```

```python
import jax
import jax.numpy as jnp
from jax import lax
from jax.experimental import pallas as pl
from jax.experimental.pallas import tpu as pltpu
from jax.sharding import Mesh, PartitionSpec as P


outer_rate = 0.7
momentum_factor = 0.9

ORDERS = ((0, 1, 2), (1, 2, 0), (2, 0, 1))
PARTS = len(ORDERS)
CUTS = (0, 352, 688, 1024)
SIZES = tuple(CUTS[k + 1] - CUTS[k] for k in range(PARTS))
BLOCK = 1024
TILE = 128


def partner(r, direction):
    y, x = r // 2, r % 2
    if direction == 0:
        y = y ^ 1
    elif direction == 1:
        y = 3 - y
    else:
        x = x ^ 1
    return 2 * y + x


def swap(v, direction):
    return lax.ppermute(v, "replica", [(r, partner(r, direction)) for r in range(8)])


def away(steps):
    r = lax.axis_index("replica")
    y, x = lax.div(r, 2), lax.rem(r, 2)
    if steps[0]:
        y = jnp.bitwise_xor(y, 1)
    if steps[1]:
        y = 3 - y
    if steps[2]:
        x = 1 - x
    return 2 * y + x


def steps_of(k, first, j):
    steps = [0, 0, 0]
    for direction, bit in zip(ORDERS[k], (first, j // 2, j % 2)):
        steps[direction] = bit
    return steps


SLOTS = tuple((s, z, c) for s in range(2) for z in range(8) for c in range(2))
WIDE = 128
TALL = 32


def mate(slot):
    s, z, c = slot
    return 4 * z + 2 * jnp.bitwise_xor(lax.axis_index("xh"), s) + c


def exchange(near, far):
    far = lax.ppermute(far, "xh", [(0, 1), (1, 0)])
    return lax.all_to_all(jnp.stack([near, far], axis=1), ("z", "c"), 0, 0, tiled=True)


def first_kernel(codes, scales, master, momentum, *refs):
    kept, sent, far_near = refs[:PARTS], refs[PARTS : 2 * PARTS], refs[2 * PARTS : 2 * PARTS + 2]
    buffer, factors, outer, sems, more = refs[2 * PARTS + 2 :]
    small = [
        pltpu.make_async_copy(master, outer.at[0], more.at[0]),
        pltpu.make_async_copy(momentum, outer.at[1], more.at[1]),
        pltpu.make_async_copy(scales, factors, more.at[2]),
    ]
    for copy in small:
        copy.start()
    copies = []
    for i in range(8):
        block = away((i // 4, i // 2 % 2, i % 2))
        start = pl.multiple_of(block * BLOCK, BLOCK)
        copy = pltpu.make_async_copy(codes.at[pl.ds(start, BLOCK)], buffer.at[i], sems.at[i])
        copy.start()
        copies.append((block, copy))
    for copy in small:
        copy.wait()
    for i, slot in enumerate(SLOTS):
        columns = pl.ds(pl.multiple_of(mate(slot) * WIDE, WIDE), WIDE)
        q = outer[0, :, columns] - (outer_rate * momentum_factor**2) * outer[1, :, columns]
        far_near[slot[0]][i % 16] = q.astype(jnp.bfloat16)
    for i, (block, copy) in enumerate(copies):
        copy.wait()
        steps = (i // 4, i // 2 % 2, i % 2)
        for tile in range(BLOCK // TILE):
            row = factors[pl.ds(block * (BLOCK // TILE) + tile, 1), :]
            factor = jnp.transpose(jnp.broadcast_to(row, (TILE, TILE)))
            base = tile * TILE
            for k, (first, second, third) in enumerate(ORDERS):
                low, high = max(base, CUTS[k]), min(base + TILE, CUTS[k + 1])
                if low < high:
                    out = (sent if steps[first] else kept)[k]
                    j = 2 * steps[second] + steps[third]
                    values = buffer[i, pl.ds(low, high - low), :].astype(jnp.float32)
                    values = values * factor[low - base : high - base]
                    out[j, pl.ds(low - CUTS[k], high - low), :] = values.astype(out.dtype)


def first(codes, scales, master, momentum):
    args = [pltpu.with_memory_space_constraint(v, pltpu.HBM) for v in (codes, scales, master, momentum)]
    out = pl.pallas_call(
        first_kernel,
        out_shape=[pltpu.VMEM((4, n, 128), jnp.bfloat16) for n in SIZES] * 2
        + [pltpu.VMEM((16, TALL, WIDE), jnp.bfloat16)] * 2,
        in_specs=[pl.BlockSpec(memory_space=pltpu.HBM)] * 4,
        out_specs=[pl.BlockSpec(memory_space=pltpu.VMEM)] * (2 * PARTS + 2),
        scratch_shapes=[
            pltpu.VMEM((8, BLOCK, 128), jnp.int32),
            pltpu.VMEM((8 * BLOCK // TILE, TILE), jnp.float32),
            pltpu.VMEM((2, *master.shape), jnp.float32),
            pltpu.SemaphoreType.DMA((8,)),
            pltpu.SemaphoreType.DMA((3,)),
        ],
        compiler_params=pltpu.CompilerParams(vmem_limit_bytes=12 << 20),
        name="first",
    )(*args)
    return list(out[:PARTS]), list(out[PARTS : 2 * PARTS]), out[2 * PARTS], out[2 * PARTS + 1]


def place_copies(pieces, first, out, sems):
    copies = []
    for k in range(PARTS):
        for j in range(4):
            start = pl.multiple_of(away(steps_of(k, first, j)) * BLOCK + CUTS[k], 16)
            rows = out.at[pl.ds(start, SIZES[k])]
            copies.append(pltpu.make_async_copy(pieces[k].at[j], rows, sems.at[k, j]))
    return copies


def place_kernel(*refs):
    copies = place_copies(refs[:PARTS], 0, *refs[PARTS:])
    for copy in copies:
        copy.start()
    for copy in copies:
        copy.wait()


def place(pieces):
    return pl.pallas_call(
        place_kernel,
        out_shape=jax.ShapeDtypeStruct((8 * BLOCK, 128), jnp.bfloat16),
        in_specs=[pl.BlockSpec(memory_space=pltpu.VMEM)] * PARTS,
        out_specs=pl.BlockSpec(memory_space=pl.ANY),
        scratch_shapes=[pltpu.SemaphoreType.DMA((PARTS, 4))],
        compiler_params=pltpu.CompilerParams(vmem_limit_bytes=4 << 20),
        name="place",
    )(*[pltpu.with_memory_space_constraint(v, pltpu.VMEM) for v in pieces])


def vmem_call(kernel, out_shape, args, limit=8):
    return pl.pallas_call(
        kernel,
        out_shape=out_shape,
        in_specs=[pl.BlockSpec(memory_space=pltpu.VMEM)] * len(args),
        out_specs=jax.tree.map(lambda _: pl.BlockSpec(memory_space=pltpu.VMEM), out_shape),
        compiler_params=pltpu.CompilerParams(vmem_limit_bytes=limit << 20),
    )(*args)


def rows_kernel(slots, out):
    for i, slot in enumerate(SLOTS):
        rows = pl.ds(pl.multiple_of(mate(slot) * TALL, TALL), TALL)
        out[rows, :] = slots[i % 16, slot[0]]


def slots_kernel(rows, near, far):
    for i, slot in enumerate(SLOTS):
        (far if slot[0] else near)[i % 16] = rows[pl.ds(pl.multiple_of(mate(slot) * TALL, TALL), TALL), :]


def add_kernel(kept, got, held, sent):
    half = kept.shape[0] // 2
    held[...] = kept[:half].astype(held.dtype) + got[:half].astype(held.dtype)
    v = kept[half:].astype(held.dtype) + got[half:].astype(held.dtype)
    sent[...] = v.astype(sent.dtype)


def last_kernel(slots, master, momentum, *refs):
    pieces, (_, out, new_master, new_momentum, sems) = refs[:PARTS], refs[PARTS:]
    copies = place_copies(pieces, 1, out, sems)
    for copy in copies:
        copy.start()
    for i, slot in enumerate(SLOTS):
        columns = pl.ds(pl.multiple_of(mate(slot) * WIDE, WIDE), WIDE)
        mean = slots[i % 16, slot[0]].astype(jnp.float32) / 8
        faster = momentum_factor * momentum[:, columns] + mean
        new_momentum[:, columns] = faster
        new_master[:, columns] = master[:, columns] - outer_rate * (mean + momentum_factor * faster)
    for copy in copies:
        copy.wait()


def last(slots, master, momentum, pieces, out):
    vmem = pl.BlockSpec(memory_space=pltpu.VMEM)
    hbm = pl.BlockSpec(memory_space=pl.ANY)
    pieces = [pltpu.with_memory_space_constraint(v, pltpu.VMEM) for v in pieces]
    return pl.pallas_call(
        last_kernel,
        out_shape=[jax.ShapeDtypeStruct(v.shape, v.dtype) for v in (out, master, momentum)],
        in_specs=[vmem] * (3 + PARTS) + [hbm],
        out_specs=[hbm, vmem, vmem],
        scratch_shapes=[pltpu.SemaphoreType.DMA((PARTS, 4))],
        input_output_aliases={3 + PARTS: 0},
        compiler_params=pltpu.CompilerParams(vmem_limit_bytes=10 << 20),
        name="last",
    )(slots, master, momentum, *pieces, out)


def step(codes, scales, master, momentum):
    f32, bf16 = jnp.float32, jnp.bfloat16
    codes, scales = codes.reshape(8 * BLOCK, 128), scales.reshape(8 * BLOCK // TILE, TILE)
    held, sent, near, far = first(codes, scales, master, momentum)
    got = []
    for k in range(PARTS):
        got.append(swap(sent[k], ORDERS[k][0]))

    q = exchange(near, far)
    for s in (1, 2):
        for k in range(PARTS):
            shape = (held[k].shape[0] // 2, *held[k].shape[1:])
            inputs = [pltpu.with_memory_space_constraint(v, pltpu.VMEM) for v in (held[k], got[k])]
            held[k], v = vmem_call(
                add_kernel, [pltpu.VMEM(shape, f32), pltpu.VMEM(shape, bf16)], inputs
            )
            got[k] = swap(v, ORDERS[k][s])
    total = [held[k][0] + got[k][0].astype(f32) for k in range(PARTS)]
    q = vmem_call(rows_kernel, pltpu.VMEM((BLOCK, WIDE), bf16), (q,))

    weights = []
    for k in range(PARTS):
        columns = q[CUTS[k] : CUTS[k + 1]].astype(f32)
        w = columns - (outer_rate * (1 + momentum_factor) / 8) * total[k]
        weights.append(w.astype(bf16)[None])
    for s in (2, 1):
        for k in range(PARTS):
            weights[k] = jnp.concatenate([weights[k], swap(weights[k], ORDERS[k][s])])
    others = []
    for k in range(PARTS):
        others.append(swap(weights[k], ORDERS[k][0]))

    near, far = vmem_call(
        slots_kernel,
        [pltpu.VMEM((16, TALL, WIDE), bf16)] * 2,
        (jnp.concatenate(total).astype(bf16),),
    )
    summed = exchange(near, far)
    out = place(weights)
    out, new_master, new_momentum = last(summed, master, momentum, others, out)
    return (new_master, new_momentum, out)


def solution(mesh):
    mesh = Mesh(mesh.devices.reshape(8, 8, 2, 2), ("replica", "z", "xh", "c"))
    fsdp = ("z", "xh", "c")
    return jax.shard_map(
        step,
        mesh=mesh,
        in_specs=(
            P("replica", None, fsdp),
            P("replica", fsdp, None),
            P(("replica", *fsdp), None),
            P(("replica", *fsdp), None),
        ),
        out_specs=(P(("replica", *fsdp), None), P(("replica", *fsdp), None), P(None, fsdp)),
        check_vma=False,
    )
```

```python
import jax
import jax.numpy as jnp
from jax import lax
from jax.experimental import pallas as pl
from jax.experimental.pallas import tpu as pltpu
from jax.sharding import Mesh, PartitionSpec as P


outer_rate = 0.7
momentum_factor = 0.9

ORDERS = ((0, 1, 2), (1, 2, 0), (2, 0, 1))
PARTS = len(ORDERS)
CUTS = (0, 384, 736, 1024)
SIZES = tuple(CUTS[k + 1] - CUTS[k] for k in range(PARTS))
BLOCK = 1024
TILE = 128


def partner(r, direction):
    y, x = r // 2, r % 2
    if direction == 0:
        y = y ^ 1
    elif direction == 1:
        y = 3 - y
    else:
        x = x ^ 1
    return 2 * y + x


def swap(v, direction):
    return lax.ppermute(v, "replica", [(r, partner(r, direction)) for r in range(8)])


def away(steps):
    r = lax.axis_index("replica")
    y, x = lax.div(r, 2), lax.rem(r, 2)
    if steps[0]:
        y = jnp.bitwise_xor(y, 1)
    if steps[1]:
        y = 3 - y
    if steps[2]:
        x = 1 - x
    return 2 * y + x


def steps_of(k, first, j):
    steps = [0, 0, 0]
    for direction, bit in zip(ORDERS[k], (first, j // 2, j % 2)):
        steps[direction] = bit
    return steps


WIDE = 128
TALL = 32


def first_kernel(codes, scales, master, momentum, *refs):
    kept, sent = refs[:PARTS], refs[PARTS : 2 * PARTS]
    q_blocks, buffer, factors, outer, ready, sems, more = refs[2 * PARTS :]
    small = [
        pltpu.make_async_copy(master, outer.at[0], more.at[0]),
        pltpu.make_async_copy(momentum, outer.at[1], more.at[1]),
        pltpu.make_async_copy(scales, factors, more.at[2]),
    ]
    for copy in small:
        copy.start()
    copies = []
    for i in range(8):
        block = away((i // 4, i // 2 % 2, i % 2))
        start = pl.multiple_of(block * BLOCK, BLOCK)
        copy = pltpu.make_async_copy(codes.at[pl.ds(start, BLOCK)], buffer.at[i], sems.at[i])
        copy.start()
        copies.append((block, copy))
    for copy in small:
        copy.wait()
    for i in range(32):
        columns = pl.ds(i * WIDE, WIDE)
        q = outer[0, :, columns] - (outer_rate * momentum_factor**2) * outer[1, :, columns]
        ready[i] = q.astype(ready.dtype)
    small.append(pltpu.make_async_copy(ready, q_blocks, more.at[3]))
    small[3].start()
    for i, (block, copy) in enumerate(copies):
        copy.wait()
        steps = (i // 4, i // 2 % 2, i % 2)
        for tile in range(BLOCK // TILE):
            row = factors[pl.ds(block * (BLOCK // TILE) + tile, 1), :]
            factor = jnp.transpose(jnp.broadcast_to(row, (TILE, TILE)))
            base = tile * TILE
            for k, (first, second, third) in enumerate(ORDERS):
                low, high = max(base, CUTS[k]), min(base + TILE, CUTS[k + 1])
                if low < high:
                    out = (sent if steps[first] else kept)[k]
                    j = 2 * steps[second] + steps[third]
                    values = buffer[i, pl.ds(low, high - low), :].astype(jnp.float32)
                    values = values * factor[low - base : high - base]
                    out[j, pl.ds(low - CUTS[k], high - low), :] = values.astype(out.dtype)
    small[3].wait()


def first(codes, scales, master, momentum):
    args = [pltpu.with_memory_space_constraint(v, pltpu.HBM) for v in (codes, scales, master, momentum)]
    out = pl.pallas_call(
        first_kernel,
        out_shape=[pltpu.VMEM((4, n, 128), jnp.bfloat16) for n in SIZES] * 2
        + [pltpu.HBM((32, TALL, WIDE), jnp.bfloat16)],
        in_specs=[pl.BlockSpec(memory_space=pltpu.HBM)] * 4,
        out_specs=[pl.BlockSpec(memory_space=pltpu.VMEM)] * (2 * PARTS)
        + [pl.BlockSpec(memory_space=pltpu.HBM)],
        scratch_shapes=[
            pltpu.VMEM((8, BLOCK, 128), jnp.int32),
            pltpu.VMEM((8 * BLOCK // TILE, TILE), jnp.float32),
            pltpu.VMEM((2, *master.shape), jnp.float32),
            pltpu.VMEM((32, TALL, WIDE), jnp.bfloat16),
            pltpu.SemaphoreType.DMA((8,)),
            pltpu.SemaphoreType.DMA((4,)),
        ],
        compiler_params=pltpu.CompilerParams(vmem_limit_bytes=12 << 20),
        name="first",
    )(*args)
    return list(out[:PARTS]), list(out[PARTS : 2 * PARTS]), out[2 * PARTS]


def place_copies(pieces, first, out, sems):
    copies = []
    for k in range(PARTS):
        for j in range(4):
            start = pl.multiple_of(away(steps_of(k, first, j)) * BLOCK + CUTS[k], 16)
            rows = out.at[pl.ds(start, SIZES[k])]
            copies.append(pltpu.make_async_copy(pieces[k].at[j], rows, sems.at[k, j]))
    return copies


def place_kernel(first, aliased):
    def kernel(*refs):
        pieces, (out, sems) = refs[aliased : aliased + PARTS], refs[aliased + PARTS :]
        copies = place_copies(pieces, first, out, sems)
        for copy in copies:
            copy.start()
        for copy in copies:
            copy.wait()

    return kernel


def place(pieces, first, out):
    aliased = [] if out is None else [out]
    return pl.pallas_call(
        place_kernel(first, len(aliased)),
        out_shape=jax.ShapeDtypeStruct((8 * BLOCK, 128), jnp.bfloat16),
        in_specs=[pl.BlockSpec(memory_space=pl.ANY)] * len(aliased)
        + [pl.BlockSpec(memory_space=pltpu.VMEM)] * PARTS,
        out_specs=pl.BlockSpec(memory_space=pl.ANY),
        scratch_shapes=[pltpu.SemaphoreType.DMA((PARTS, 4))],
        input_output_aliases={0: 0} if aliased else {},
        compiler_params=pltpu.CompilerParams(vmem_limit_bytes=4 << 20),
    )(*aliased, *[pltpu.with_memory_space_constraint(v, pltpu.VMEM) for v in pieces])


def vmem_call(kernel, out_shape, args, limit=8):
    return pl.pallas_call(
        kernel,
        out_shape=out_shape,
        in_specs=[pl.BlockSpec(memory_space=pltpu.VMEM)] * len(args),
        out_specs=jax.tree.map(lambda _: pl.BlockSpec(memory_space=pltpu.VMEM), out_shape),
        compiler_params=pltpu.CompilerParams(vmem_limit_bytes=limit << 20),
    )(*args)


def add_kernel(kept, got, held, sent):
    half = kept.shape[0] // 2
    held[...] = kept[:half].astype(held.dtype) + got[:half].astype(held.dtype)
    v = kept[half:].astype(held.dtype) + got[half:].astype(held.dtype)
    sent[...] = v.astype(sent.dtype)


def update_kernel(blocks, master, momentum, new_master, new_momentum):
    for i in range(32):
        columns = pl.ds(i * WIDE, WIDE)
        mean = blocks[i].astype(jnp.float32) / 8
        faster = momentum_factor * momentum[:, columns] + mean
        new_momentum[:, columns] = faster
        new_master[:, columns] = master[:, columns] - outer_rate * (mean + momentum_factor * faster)


def step(codes, scales, master, momentum):
    f32, bf16 = jnp.float32, jnp.bfloat16
    codes, scales = codes.reshape(8 * BLOCK, 128), scales.reshape(8 * BLOCK // TILE, TILE)
    held, sent, q = first(codes, scales, master, momentum)
    got = []
    for k in range(PARTS):
        got.append(swap(sent[k], ORDERS[k][0]))

    q = lax.all_to_all(q, ("z", "xh", "c"), 0, 0, tiled=True).reshape(BLOCK, WIDE)
    for s in (1, 2):
        for k in range(PARTS):
            shape = (held[k].shape[0] // 2, *held[k].shape[1:])
            inputs = [pltpu.with_memory_space_constraint(v, pltpu.VMEM) for v in (held[k], got[k])]
            held[k], v = vmem_call(add_kernel, [pltpu.VMEM(shape, f32), pltpu.VMEM(shape, bf16)], inputs)
            got[k] = swap(v, ORDERS[k][s])
    total = [held[k][0] + got[k][0].astype(f32) for k in range(PARTS)]
    weights = []
    for k in range(PARTS):
        columns = q[CUTS[k] : CUTS[k + 1]].astype(f32)
        w = columns - (outer_rate * (1 + momentum_factor) / 8) * total[k]
        weights.append(w.astype(bf16)[None])
    for s in (2, 1):
        for k in range(PARTS):
            weights[k] = jnp.concatenate([weights[k], swap(weights[k], ORDERS[k][s])])
    others = []
    for k in range(PARTS):
        others.append(swap(weights[k], ORDERS[k][0]))

    summed = jnp.concatenate(total).astype(bf16).reshape(32, TALL, WIDE)
    summed = lax.all_to_all(summed, ("z", "xh", "c"), 0, 0, tiled=True)
    out = place(weights, 0, None)
    new_master, new_momentum = vmem_call(
        update_kernel, [jax.ShapeDtypeStruct(master.shape, f32)] * 2, (summed, master, momentum)
    )
    out = place(others, 1, out)
    return (new_master, new_momentum, out)


def solution(mesh):
    mesh = Mesh(mesh.devices.reshape(8, 8, 2, 2), ("replica", "z", "xh", "c"))
    fsdp = ("z", "xh", "c")
    return jax.shard_map(
        step,
        mesh=mesh,
        in_specs=(
            P("replica", None, fsdp),
            P("replica", fsdp, None),
            P(("replica", *fsdp), None),
            P(("replica", *fsdp), None),
        ),
        out_specs=(P(("replica", *fsdp), None), P(("replica", *fsdp), None), P(None, fsdp)),
        check_vma=False,
    )
```
